32 devices in a mesh: seq: 2 (over x), expert: 16 (over z, y, core).
Axes of the slice: x: 2, y: 2, z: 4, core: 2. Of those that a mesh axis runs over, the one named last changes fastest.
Arguments:
- tokens: bfloat16 [768, 7168], P('expert', 'seq'), may hold values from -6 to 6
- expert_ids: int32 [768, 8], P('expert'), may hold values from 0 to 15, all different within a row
- route_weights: float32 [768, 8], P('expert'), may hold values from 0.05 to 1
- capacity: int32 [16], replicated, may hold values from 6 to 12
- expert_gate_up: bfloat16 [16, 2, 1024, 7168], P('expert', None, 'seq'), may hold values from -0.0625 to 0.0625
- expert_down: bfloat16 [16, 1024, 7168], P('expert', None, 'seq'), may hold values from -0.1875 to 0.1875
Outputs:
- mixed: bfloat16 [768, 7168], P('expert', 'seq')
The draws below stay inside these ranges and needn't reach their ends.
Inputs may be any that keep to these rules, and one draw needn't show every extreme that they name: `expert_ids`: each row names 8 different experts.
All inputs are finite; a program needn't handle non-finite values.
Results may differ from the reference program's by a relative error of at most 0.02.
Values may be sent and summed in bfloat16 or wider, within the bound.
A program may use at most 128 MiB of HBM per device.

```python
import math
import jax
import jax.numpy as jnp
from jax import lax

D = 7168
TOP = 8
FF = 1024
TG = 48
CAP = 12
EXPERTS = 16
TOKENS = 768
N_SEQ = 2


def place_ends(result, rng, least, largest):
    extent = result.shape
    index_at = [jax.random.randint(jax.random.fold_in(rng, axis), (), 0, extent[axis]) for axis in range(len(extent))]
    result = result.at[tuple(index_at)].set(least)
    longest = extent.index(max(extent))
    index_at[longest] = (index_at[longest] + 1) % extent[longest]
    return result.at[tuple(index_at)].set(largest)


def shard_levels(stream_key, dims, shards, smallest, largest):
    loudness, own = 1.0, jax.random.fold_in(stream_key, 6)
    for dim, shards_of in shards:
        draws = jnp.exp(jax.random.uniform(jax.random.fold_in(own, dim), (shards_of,), jnp.float32, smallest / len(shards), largest / len(shards)))
        loudness = loudness * jnp.repeat(draws, dims[dim] // shards_of).reshape([-1 if axis == dim else 1 for axis in range(len(dims))])
    return loudness


def choose_distinct(own_key, rows, count, top, lift):
    ranking = jax.random.permutation(jax.random.fold_in(own_key, 1), count)
    boost = ranking
    for power in range(3):
        boost = boost * boost // count
    boost = boost * lift // count
    lots = jax.random.randint(jax.random.fold_in(own_key, 2), (rows, count), 0, 4096) + boost
    sure = jax.random.permutation(jax.random.fold_in(own_key, 3), rows)[jnp.arange(count) % rows]
    lots = jnp.where(jnp.arange(rows)[:, None] == sure[None, :], 1 << 14, lots)
    score = lots * count + jnp.arange(count)
    return lax.top_k(score.astype(jnp.int32), top)[1].astype(jnp.int32)


def gaussian(own_key, shape, scale, bound, shards=(), kind=jnp.bfloat16):
    gain = shard_levels(own_key, shape, shards, -0.22, 0.18) if shards else 1.0
    array = jax.random.normal(own_key, shape, jnp.float32) * scale * gain
    return jnp.minimum(jnp.maximum(array, -bound), bound).astype(kind)


def setup_inputs(seed: int = 0) -> dict:
    seeds = jax.random.split(jax.random.key(seed), 7)
    tokens = gaussian(seeds[0], (TOKENS, D), 1.0, 6.0, ((0, 16), (1, 2)))
    expert_ids = choose_distinct(seeds[1], TOKENS, EXPERTS, TOP, 8192)
    route_weights = jnp.clip(jnp.exp(math.log(1.0) - 2.9957323 * jax.random.uniform(seeds[2], (TOKENS, TOP), jnp.float32) ** shard_levels(seeds[2], (TOKENS, TOP), ((0, 16),), -0.2, 0.2)), 0.05, 1.0)
    capacity = place_ends(jax.random.randint(seeds[3], (EXPERTS,), max(1, CAP // 2), CAP + 1), jax.random.fold_in(seeds[3], 1), max(1, CAP // 2), CAP).astype(jnp.int32)
    expert_gate_up = gaussian(seeds[4], (EXPERTS, 2, FF, D), D ** -0.5, 0.0625, ((0, 16), (2, 2)))
    expert_down = gaussian(seeds[5], (EXPERTS, FF, D), FF ** -0.5, 0.1875, ((0, 16), (2, 2)))
    return {"tokens": tokens, "expert_ids": expert_ids, "route_weights": route_weights, "capacity": capacity, "expert_gate_up": expert_gate_up, "expert_down": expert_down}


def reference(tokens, expert_ids, route_weights, capacity, expert_gate_up, expert_down):
    token_count = tokens.shape[0]
    width = tokens.shape[1]
    top_count = expert_ids.shape[1]
    expert_count = capacity.shape[0]
    group_count = token_count // TG
    assign = TG * top_count
    block_width = width // N_SEQ
    flat_ids = expert_ids.reshape(group_count, assign)
    one_hot = (flat_ids[:, :, None] == jnp.arange(expert_count, dtype=jnp.int32)[None, None, :]).astype(jnp.int32)
    within = jnp.sum((jnp.cumsum(one_hot, axis=1) - one_hot) * one_hot, axis=2).astype(jnp.int32)
    retained = within < capacity[flat_ids]
    token_index = (jnp.arange(group_count, dtype=jnp.int32)[:, None] * TG
                   + jnp.arange(assign, dtype=jnp.int32)[None, :] // top_count).astype(jnp.int32)
    group_index = jnp.broadcast_to(jnp.arange(group_count, dtype=jnp.int32)[:, None], (group_count, assign))
    target = jnp.where(retained, flat_ids, expert_count).astype(jnp.int32)
    place = jnp.minimum(within, CAP - 1).astype(jnp.int32)
    table = jnp.full((expert_count, group_count, CAP), token_count, jnp.int32)
    table = table.at[target, group_index, place].set(token_index, mode="drop")
    padded = jnp.concatenate([tokens, jnp.zeros((1, width), jnp.bfloat16)], axis=0)
    weight_flat = jnp.where(retained, route_weights.reshape(group_count, assign), 0.0).astype(jnp.float32)
    column = (group_index * CAP + within).astype(jnp.int32)
    column = jnp.where(retained, column, group_count * CAP).astype(jnp.int32)

    def project(rows, weight):
        blocks = rows.reshape(rows.shape[0], N_SEQ, block_width)
        wblocks = weight.astype(jnp.float32).reshape(weight.shape[0], N_SEQ, block_width)
        partial_value = jnp.einsum("nsd,fsd->snf", blocks, wblocks)
        rounded = lax.optimization_barrier(partial_value.astype(jnp.bfloat16))
        return jnp.sum(rounded.astype(jnp.float32), axis=0)

    def one_expert(total, expert):
        rows = padded[table[expert].reshape(-1)].astype(jnp.float32)
        gate = project(rows, expert_gate_up[expert, 0])
        up = project(rows, expert_gate_up[expert, 1])
        hidden = (jax.nn.silu(gate) * up).astype(jnp.bfloat16)
        output = jnp.dot(hidden.astype(jnp.float32), expert_down[expert].astype(jnp.float32),
                         preferred_element_type=jnp.float32).astype(jnp.bfloat16)
        select = jnp.where(flat_ids == expert, weight_flat, 0.0).astype(jnp.float32)
        mixing = jnp.zeros((token_count, group_count * CAP), jnp.float32)
        mixing = mixing.at[token_index.reshape(-1), column.reshape(-1)].add(select.reshape(-1), mode="drop")
        total = total + jnp.dot(mixing, output.astype(jnp.float32), precision=lax.Precision.HIGHEST)
        return total, None

    total, _ = lax.scan(one_expert, jnp.zeros((token_count, width), jnp.float32),
                        jnp.arange(expert_count, dtype=jnp.int32))
    return total.astype(jnp.bfloat16)
```

```python
import functools

import jax
import jax.numpy as jnp
from jax import lax
from jax.experimental import pallas as pl
from jax.experimental.pallas import tpu as pltpu
from jax.sharding import PartitionSpec as P

CAP = 12
MESH = pl.DeviceIdType.MESH
F32 = jnp.float32
BF16 = jnp.bfloat16


def kernel(
    n_seq, n_expert, info_ref, tokens_ref, gate_up_ref, down_ref, out_ref,
    wgu, wdn, tok, info, xr, hb, mine, pout, dd, sr, sl, rr, ll,
    local_sem, info_s, info_r, ag_s, ag_r, tw_s, tw_r, x_s, x_r, h_s, h_r, p_s, p_r, rs_s, rs_r,
):
    chips = n_expert // 2
    far = chips // 2
    group, half = tok.shape[3], tok.shape[4]
    share = 2 * half
    hid = wgu.shape[1]
    me_e = lax.axis_index("expert")
    me_s = lax.axis_index("seq")
    core = lax.rem(me_e, 2)
    chip = lax.div(me_e, 2)
    odd = lax.rem(chip, 2)
    pos = (1 - odd) * lax.div(chip, 2) + odd * (chips - 1 - lax.div(chip, 2))

    def device_at(offset, same_core):
        at = lax.rem(pos + offset + 2 * chips, chips)
        back = lax.div(at, far)
        there = (1 - back) * 2 * at + back * (2 * (chips - 1 - at) + 1)
        return there * 2 + (core if same_core else 1 - core)

    right, left, twin = device_at(1, True), device_at(-1, True), device_at(0, False)

    def remote(src, dst, send, recv, device):
        return pltpu.make_async_remote_copy(
            src_ref=src, dst_ref=dst, send_sem=send, recv_sem=recv,
            device_id=device, device_id_type=MESH,
        )

    def info_copy(d, cr):
        to = device_at(-d, cr == 0)
        return remote(info_ref.at[to], info.at[d, cr], info_s.at[d, cr], info_r.at[d, cr], {"expert": to})

    def gather_copy(way, k, h):
        src = lax.rem(chips - k + 1, chips) if way == 0 else k - 1
        dst = chips - k if way == 0 else k
        return remote(
            tok.at[src, 0, h], tok.at[dst, 0, h], ag_s.at[way, k - 1, h], ag_r.at[way, k - 1, h],
            {"expert": right if way == 0 else left},
        )

    def twin_copy(d, h):
        return remote(tok.at[d, 0, h], tok.at[d, 1, h], tw_s.at[d, h], tw_r.at[d, h], {"expert": twin})

    def rows_copy(k, o, receive=False):
        slot = lax.rem(me_s - o + n_seq, n_seq) if receive else me_s
        return remote(
            xr.at[k - 1, slot], xr.at[k - 1, slot], x_s.at[k - 1, o - 1], x_r.at[k - 1, o - 1],
            {"seq": lax.rem(me_s + o, n_seq)},
        )

    def hidden_copy(k, o, receive=False):
        slot = lax.rem(me_s - o + n_seq, n_seq) if receive else me_s
        return remote(
            hb.at[k - 1, slot], hb.at[k - 1, slot], h_s.at[k - 1, o - 1], h_r.at[k - 1, o - 1],
            {"seq": lax.rem(me_s + o, n_seq)},
        )

    def partial_copy(d, h):
        return remote(pout.at[d, h], dd.at[d, h], p_s.at[d, h], p_r.at[d, h], {"expert": twin})

    def sum_copy(way, k, h):
        src, dst = (sr, rr) if way == 0 else (sl, ll)
        return remote(
            src.at[k - 1, h], dst.at[k - 1, h], rs_s.at[way, k - 1, h], rs_r.at[way, k - 1, h],
            {"expert": right if way == 0 else left},
        )

    load_tokens = pltpu.make_async_copy(tokens_ref, tok.at[0, 0], local_sem.at[0])
    load_info = pltpu.make_async_copy(info_ref.at[me_e], info.at[0, 0], local_sem.at[1])
    load_gu = pltpu.make_async_copy(gate_up_ref, wgu, local_sem.at[2])
    load_dn = pltpu.make_async_copy(down_ref, wdn, local_sem.at[3])
    load_tokens.start()
    load_info.start()
    load_gu.start()
    load_dn.start()

    barrier = pltpu.get_barrier_semaphore()
    for o in range(1, n_expert):
        pl.semaphore_signal(
            barrier, inc=1, device_id={"expert": lax.rem(me_e + o, n_expert)}, device_id_type=MESH
        )
    for o in range(1, n_seq):
        pl.semaphore_signal(
            barrier, inc=1, device_id={"seq": lax.rem(me_s + o, n_seq)}, device_id_type=MESH
        )
    load_tokens.wait()
    load_info.wait()
    pl.semaphore_wait(barrier, n_expert - 1 + n_seq - 1)

    others = [(d, cr) for d in range(chips) for cr in range(2) if d or cr]
    for way, h in ((0, 0), (1, 1), (0, 1), (1, 0)):
        gather_copy(way, 1, h).start()
    for h in range(2):
        twin_copy(0, h).start()
    for d, cr in others:
        info_copy(d, cr).start()

    def pair(k):
        return k, (chips - k) * (1 - lax.div(k, far))

    def slots_of(k, weighted):
        first, second = pair(k)
        parts = []
        for j, (d, cr) in enumerate(((first, 0), (first, 1), (second, 0), (second, 1))):
            block = info[d, cr]
            rank = block[1:2, :group]
            row = lax.broadcasted_iota(jnp.int32, (4 * CAP, group), 0).astype(F32)
            hit = row == rank + float(CAP * j)
            parts.append(jnp.where(hit, block[0:1, :group] if weighted else 1.0, 0.0))
        return jnp.concatenate(parts, axis=1).astype(BF16)

    def select(k, last):
        first, second = pair(k)
        placing = slots_of(k, False)
        for h in range(2):
            block = jnp.concatenate(
                [tok[first, 0, h], tok[first, 1, h], tok[second, 0, h], tok[second, 1, h]], axis=0
            )
            xr[k - 1, me_s, h] = jnp.dot(placing, block, preferred_element_type=F32).astype(BF16)
        for o in range(1, n_seq):
            rows_copy(k, o).start()

    def gate_up(k):
        for o in range(1, n_seq):
            rows_copy(k, o, True).wait_recv()
        tile = min(hid, 256)
        for n in range(hid // tile):
            sums = []
            for g in range(2):
                total = None
                for s in range(n_seq):
                    part = None
                    for h in range(2):
                        at = s * share + h * half
                        term = lax.dot_general(
                            xr[k - 1, s, h], wgu[g, n * tile:(n + 1) * tile, at:at + half],
                            (((1,), (1,)), ((), ())), preferred_element_type=F32,
                        )
                        part = term if part is None else part + term
                    part = part.astype(BF16).astype(F32)
                    total = part if total is None else total + part
                sums.append(total)
            value = sums[0] / (1.0 + jnp.exp(-sums[0])) * sums[1]
            hb[k - 1, me_s, :, n * tile:(n + 1) * tile] = value.astype(BF16)
        for o in range(1, n_seq):
            hidden_copy(k, o).start()

    def down(k):
        for o in range(1, n_seq):
            hidden_copy(k, o, True).wait_recv()
        first, second = pair(k)
        mixing = slots_of(k, True).astype(F32).T.astype(BF16)
        for h in range(2):
            value = None
            for s in range(n_seq):
                term = jnp.dot(
                    hb[k - 1, s], wdn[s * hid:(s + 1) * hid, h * half:(h + 1) * half],
                    preferred_element_type=F32,
                )
                value = term if value is None else value + term
            mixed = jnp.dot(mixing, value.astype(BF16), preferred_element_type=F32).astype(BF16)
            mine[first, h] = mixed[:group]
            pout[first, h] = mixed[group:2 * group]
            mine[second, h] = mixed[2 * group:3 * group]
            pout[second, h] = mixed[3 * group:]
            partial_copy(first, h).start()
            partial_copy(second, h).start()

    for d, cr in others:
        info_copy(d, cr).wait_recv()
    for h in range(2):
        twin_copy(0, h).wait_recv()

    def arrive(way, k, h, forward):
        gather_copy(way, k, h).wait_recv()
        if forward is not None:
            @pl.when(forward)
            def _():
                gather_copy(way, k + 1, h).start()
        twin_copy(chips - k if way == 0 else k, h).start()

    def gather_step(k, carry):
        arrive(0, k, 0, k < far)
        arrive(1, k, 1, k < far)

        @pl.when(k == 3)
        def _():
            load_gu.wait()

        @pl.when(k >= 3)
        def _():
            gate_up(k - 2)

        arrive(0, k, 1, k < far - 1)
        arrive(1, k, 0, k < far - 1)
        for h in range(2):
            twin_copy(k, h).wait_recv()
            twin_copy(chips - k, h).wait_recv()
        select(k, False)
        return carry

    lax.fori_loop(1, far, gather_step, 0)
    if far <= 3:
        load_gu.wait()
    arrive(0, far, 0, None)
    arrive(1, far, 1, None)
    for h in range(2):
        twin_copy(far, h).wait_recv()
    select(far, True)
    load_dn.wait()

    def up_step(k, carry):
        gate_up(k)
        return carry

    def down_step(k, carry):
        down(k)
        return carry

    lax.fori_loop(max(1, far - 2), far, up_step, 0)
    lax.fori_loop(1, far, down_step, 0)
    gate_up(far)
    down(far)

    for k in range(far, 0, -1):
        for way, h in ((0, 1), (1, 0), (0, 0), (1, 1)):
            if k == far and h != way:
                continue
            d = k if way == 0 else chips - k
            partial_copy(d, h).wait_recv()
            value = mine[d, h].astype(F32) + dd[d, h].astype(F32)
            if k + 1 < far or (k + 1 == far and h == way):
                sum_copy(way, k + 1, h).wait_recv()
                value = value + (rr if way == 0 else ll)[k, h].astype(F32)
            (sr if way == 0 else sl)[k - 1, h] = value.astype(BF16)
            sum_copy(way, k, h).start()
    for h in range(2):
        partial_copy(0, h).wait_recv()
        value = mine[0, h].astype(F32) + dd[0, h].astype(F32)
        sum_copy(0, 1, h).wait_recv()
        sum_copy(1, 1, h).wait_recv()
        value = value + rr[0, h].astype(F32) + ll[0, h].astype(F32)
        out_ref[:, h * half:(h + 1) * half] = value.astype(BF16)

    for d, cr in others:
        info_copy(d, cr).wait_send()
    for k in range(1, far + 1):
        for way in range(2):
            for h in range(2):
                if k < far or h == way:
                    gather_copy(way, k, h).wait_send()
                    sum_copy(way, k, h).wait_send()
        for o in range(1, n_seq):
            rows_copy(k, o).wait_send()
            hidden_copy(k, o).wait_send()
    for d in range(chips):
        for h in range(2):
            twin_copy(d, h).wait_send()
            partial_copy(d, h).wait_send()


def body(n_seq, n_expert, tokens, expert_ids, route_weights, capacity, expert_gate_up, expert_down):
    group, share = tokens.shape
    half = share // 2
    hid, width = expert_gate_up.shape[2:]
    units = expert_down.shape[1]
    chips = n_expert // 2
    far = chips // 2
    hit = expert_ids[None, :, :] == jnp.arange(n_expert, dtype=jnp.int32)[:, None, None]
    weight = jnp.sum(jnp.where(hit, route_weights[None], 0.0), axis=2)
    chosen = jnp.any(hit, axis=2)
    earlier = jnp.arange(group)[:, None] < jnp.arange(group)[None, :]
    rank = jnp.dot(chosen.astype(BF16), earlier.astype(BF16), preferred_element_type=F32)
    keep = jnp.logical_and(chosen, rank < capacity.astype(F32)[:, None])
    table = jnp.stack([jnp.where(keep, weight, 0.0), jnp.where(keep, rank, -10000.0)], axis=1)
    table = jnp.pad(table, ((0, 0), (0, 6), (0, -group % 128)))
    blocks = tokens.reshape(group, 2, half).transpose(1, 0, 2)
    sem = pltpu.SemaphoreType.DMA
    rows = 4 * CAP
    block = (group, half)
    return pl.pallas_call(
        functools.partial(kernel, n_seq, n_expert),
        out_shape=jax.ShapeDtypeStruct((group, share), BF16),
        in_specs=[
            pl.BlockSpec(memory_space=pltpu.VMEM),
            pl.BlockSpec(memory_space=pl.ANY),
            pl.BlockSpec(memory_space=pl.ANY),
            pl.BlockSpec(memory_space=pl.ANY),
        ],
        out_specs=pl.BlockSpec(memory_space=pltpu.VMEM),
        scratch_shapes=[
            pltpu.VMEM((2, hid, width), BF16),
            pltpu.VMEM((units, share), BF16),
            pltpu.VMEM((chips, 2, 2) + block, BF16),
            pltpu.VMEM((chips, 2, 8, table.shape[2]), F32),
            pltpu.VMEM((far, n_seq, 2, rows, half), BF16),
            pltpu.VMEM((far, n_seq, rows, hid), BF16),
            pltpu.VMEM((chips, 2) + block, BF16),
            pltpu.VMEM((chips, 2) + block, BF16),
            pltpu.VMEM((chips, 2) + block, BF16),
            pltpu.VMEM((far, 2) + block, BF16),
            pltpu.VMEM((far, 2) + block, BF16),
            pltpu.VMEM((far, 2) + block, BF16),
            pltpu.VMEM((far, 2) + block, BF16),
            sem((4,)),
            sem((chips, 2)), sem((chips, 2)),
            sem((2, far, 2)), sem((2, far, 2)),
            sem((chips, 2)), sem((chips, 2)),
            sem((far, max(1, n_seq - 1))), sem((far, max(1, n_seq - 1))),
            sem((far, max(1, n_seq - 1))), sem((far, max(1, n_seq - 1))),
            sem((chips, 2)), sem((chips, 2)),
            sem((2, far, 2)), sem((2, far, 2)),
        ],
        compiler_params=pltpu.CompilerParams(
            collective_id=0, has_side_effects=True, vmem_limit_bytes=60 * 1024 * 1024
        ),
    )(table, blocks, expert_gate_up[0], expert_down[0])


def solution(mesh):
    in_specs = (
        P("expert", "seq"),
        P("expert", None),
        P("expert", None),
        P(),
        P("expert", None, "seq", None),
        P("expert", None, "seq"),
    )
    return jax.shard_map(
        functools.partial(body, mesh.shape["seq"], mesh.shape["expert"]),
        mesh=mesh, in_specs=in_specs, out_specs=P("expert", "seq"), check_vma=False,
    )
```

```python
import functools

import jax
import jax.numpy as jnp
from jax import lax
from jax.experimental import pallas as pl
from jax.experimental.pallas import tpu as pltpu
from jax.sharding import PartitionSpec as P

CAP = 12
MESH = pl.DeviceIdType.MESH
F32 = jnp.float32
BF16 = jnp.bfloat16


def kernel(
    n_seq, n_expert, ids_ref, weight_ref, cap_ref, tokens_ref, gate_up_ref, down_ref, out_ref,
    wgu, wdn, tok, table, info, xr, acc, hb, mine, pout, dd, sr, sl, rr, ll,
    local_sem, info_s, info_r, ag_s, ag_r, tw_s, tw_r, x_s, x_r, h_s, h_r, p_s, p_r, rs_s, rs_r,
):
    chips = n_expert // 2
    far = chips // 2
    group, half = tok.shape[3], tok.shape[4]
    share = 2 * half
    hid = wgu.shape[1]
    rows = xr.shape[3]
    small = -(-2 * CAP // 16) * 16
    aligned = half % 128 == 0
    me_e = lax.axis_index("expert")
    me_s = lax.axis_index("seq")
    core = lax.rem(me_e, 2)
    chip = lax.div(me_e, 2)
    odd = lax.rem(chip, 2)
    pos = (1 - odd) * lax.div(chip, 2) + odd * (chips - 1 - lax.div(chip, 2))

    def device_at(offset, same_core):
        at = lax.rem(pos + offset + 2 * chips, chips)
        back = lax.div(at, far)
        there = (1 - back) * 2 * at + back * (2 * (chips - 1 - at) + 1)
        return there * 2 + (core if same_core else 1 - core)

    right, left, twin = device_at(1, True), device_at(-1, True), device_at(0, False)

    def remote(src, dst, send, recv, device):
        return pltpu.make_async_remote_copy(
            src_ref=src, dst_ref=dst, send_sem=send, recv_sem=recv,
            device_id=device, device_id_type=MESH,
        )

    def info_copy(d, cr):
        to = device_at(-d, cr == 0)
        return remote(table.at[to], info.at[d, cr], info_s.at[d, cr], info_r.at[d, cr], {"expert": to})

    def gather_copy(way, k, h):
        src = lax.rem(chips - k + 1, chips) if way == 0 else k - 1
        dst = chips - k if way == 0 else k
        return remote(
            tok.at[src, 0, h], tok.at[dst, 0, h], ag_s.at[way, k - 1, h], ag_r.at[way, k - 1, h],
            {"expert": right if way == 0 else left},
        )

    def twin_copy(d, h):
        return remote(tok.at[d, 0, h], tok.at[d, 1, h], tw_s.at[d, h], tw_r.at[d, h], {"expert": twin})

    def rows_copy(k, h, o, single, receive=False):
        slot = lax.rem(me_s - o + n_seq, n_seq) if receive else me_s
        span = xr.at[k, slot, h, pl.ds(0, small)] if single else xr.at[k, slot, h]
        return remote(
            span, span, x_s.at[k, h, o - 1], x_r.at[k, h, o - 1], {"seq": lax.rem(me_s + o, n_seq)}
        )

    def hidden_copy(k, o, receive=False):
        slot = lax.rem(me_s - o + n_seq, n_seq) if receive else me_s
        return remote(
            hb.at[k, slot], hb.at[k, slot], h_s.at[k, o - 1], h_r.at[k, o - 1],
            {"seq": lax.rem(me_s + o, n_seq)},
        )

    def partial_copy(d, h):
        return remote(pout.at[d, h], dd.at[d, h], p_s.at[d, h], p_r.at[d, h], {"expert": twin})

    def sum_copy(way, k, h):
        src, dst = (sr, rr) if way == 0 else (sl, ll)
        return remote(
            src.at[k - 1, h], dst.at[k - 1, h], rs_s.at[way, k - 1, h], rs_r.at[way, k - 1, h],
            {"expert": right if way == 0 else left},
        )

    if aligned:
        load_tokens = [
            pltpu.make_async_copy(
                tokens_ref.at[:, pl.ds(h * half, half)], tok.at[0, 0, h], local_sem.at[h]
            )
            for h in range(2)
        ]
    else:
        load_tokens = [pltpu.make_async_copy(tokens_ref, tok.at[0, 0], local_sem.at[0])]
    load_gu = pltpu.make_async_copy(gate_up_ref, wgu, local_sem.at[2])
    load_dn = pltpu.make_async_copy(down_ref, wdn, local_sem.at[3])
    for load in load_tokens:
        load.start()
    load_gu.start()
    load_dn.start()

    barrier = pltpu.get_barrier_semaphore()
    for o in range(1, n_expert):
        pl.semaphore_signal(
            barrier, inc=1, device_id={"expert": lax.rem(me_e + o, n_expert)}, device_id_type=MESH
        )
    for o in range(1, n_seq):
        pl.semaphore_signal(
            barrier, inc=1, device_id={"seq": lax.rem(me_s + o, n_seq)}, device_id_type=MESH
        )
    expert_at = lax.broadcasted_iota(jnp.int32, (n_expert, group), 0)
    weight = jnp.zeros((n_expert, group), F32)
    chosen = jnp.zeros((n_expert, group), F32)
    for c in range(ids_ref.shape[0]):
        hit = expert_at == ids_ref[c:c + 1, :]
        weight = weight + jnp.where(hit, weight_ref[c:c + 1, :], 0.0)
        chosen = chosen + jnp.where(hit, 1.0, 0.0)
    before = lax.broadcasted_iota(jnp.int32, (group, group), 0)
    after = lax.broadcasted_iota(jnp.int32, (group, group), 1)
    earlier = jnp.where(before < after, 1.0, 0.0).astype(BF16)
    rank = jnp.dot(chosen.astype(BF16), earlier, preferred_element_type=F32)
    limit = jnp.zeros((n_expert, group), jnp.int32)
    for e in range(n_expert):
        limit = jnp.where(expert_at == e, cap_ref[e], limit)
    keep = jnp.logical_and(chosen > 0.5, rank < limit.astype(F32))
    weight = jnp.where(keep, weight, 0.0)
    rank = jnp.where(keep, rank, -10000.0)
    for e in range(n_expert):
        table[e, 0:1, :group] = weight[e:e + 1]
        table[e, 1:2, :group] = rank[e:e + 1]
    info[0, 0] = table[me_e]
    for k in (0, far):
        for s in range(n_seq):
            for h in range(2):
                xr[k, s, h, small:] = jnp.zeros((rows - small, half), BF16)
    for load in load_tokens:
        load.wait()
    pl.semaphore_wait(barrier, n_expert - 1 + n_seq - 1)

    others = [(d, cr) for d in range(chips) for cr in range(2) if d or cr]
    for way, h in ((0, 0), (1, 0), (0, 1), (1, 1)):
        gather_copy(way, 1, h).start()
    for h in range(2):
        twin_copy(0, h).start()
    for d, cr in others:
        info_copy(d, cr).start()

    def distances(k, single):
        return (k,) if single else (k, chips - k)

    def slots_of(k, single, weighted, height):
        parts = []
        for d in distances(k, single):
            for cr in range(2):
                block = info[d, cr]
                row = lax.broadcasted_iota(jnp.int32, (height, group), 0).astype(F32)
                hit = row == block[1:2, :group] + float(CAP * len(parts))
                parts.append(jnp.where(hit, block[0:1, :group] if weighted else 1.0, 0.0))
        return jnp.concatenate(parts, axis=1)

    def select(k, h, single):
        height = small if single else rows
        placing = slots_of(k, single, False, height).astype(BF16)
        for d in distances(k, single):
            twin_copy(d, h).wait_recv()
        block = jnp.concatenate([tok[d, cr, h] for d in distances(k, single) for cr in range(2)], axis=0)
        xr[k, me_s, h, :height] = jnp.dot(placing, block, preferred_element_type=F32).astype(BF16)
        for o in range(1, n_seq):
            rows_copy(k, h, o, single).start()

    def take_info(k, single):
        for d in distances(k, single):
            info_copy(d, 1).wait_recv()
            if not (single and isinstance(d, int) and d == 0):
                info_copy(d, 0).wait_recv()

    def block_sum(k, s, dynamic):
        total = None
        for h in range(2):
            at = s * share + h * half
            columns = pl.ds(pl.multiple_of(at, 128), half) if dynamic else slice(at, at + half)
            term = [
                lax.dot_general(
                    xr[k, s, h], wgu[g, :, columns], (((1,), (1,)), ((), ())),
                    preferred_element_type=F32,
                )
                for g in range(2)
            ]
            total = term if total is None else [a + b for a, b in zip(total, term)]
        return [a.astype(BF16).astype(F32) for a in total]

    def gate_own(k):
        if aligned:
            own = block_sum(k, me_s, True)
            for g in range(2):
                acc[k, g] = own[g]

    def gate_rest(k, single):
        for o in range(1, n_seq):
            for h in range(2):
                rows_copy(k, h, o, single, True).wait_recv()
        if aligned:
            total = [acc[k, g] for g in range(2)]
            for o in range(1, n_seq):
                more = block_sum(k, lax.rem(me_s - o + n_seq, n_seq), True)
                total = [a + b for a, b in zip(total, more)]
        else:
            total = block_sum(k, 0, False)
            for s in range(1, n_seq):
                total = [a + b for a, b in zip(total, block_sum(k, s, False))]
        value = total[0] / (1.0 + jnp.exp(-total[0])) * total[1]
        hb[k, me_s] = value.astype(BF16)
        for o in range(1, n_seq):
            hidden_copy(k, o).start()

    def down(k, single):
        for o in range(1, n_seq):
            hidden_copy(k, o, True).wait_recv()
        mixing = slots_of(k, single, True, rows).T.astype(BF16)
        for h in range(2):
            value = None
            for s in range(n_seq):
                term = jnp.dot(
                    hb[k, s], wdn[s * hid:(s + 1) * hid, h * half:(h + 1) * half],
                    preferred_element_type=F32,
                )
                value = term if value is None else value + term
            mixed = jnp.dot(mixing, value.astype(BF16), preferred_element_type=F32).astype(BF16)
            for j, d in enumerate(distances(k, single)):
                mine[d, h] = mixed[2 * j * group:(2 * j + 1) * group]
                pout[d, h] = mixed[(2 * j + 1) * group:(2 * j + 2) * group]
                partial_copy(d, h).start()

    def arrive(way, k, h, forward):
        gather_copy(way, k, h).wait_recv()
        if forward is not None:
            @pl.when(forward)
            def _():
                gather_copy(way, k + 1, h).start()
        twin_copy(chips - k if way == 0 else k, h).start()

    take_info(0, True)
    for h in range(2):
        select(0, h, True)

    def gather_step(k, carry):
        arrive(0, k, 0, k < far)
        arrive(1, k, 0, k < far - 1)
        take_info(k, False)
        select(k, 0, False)

        @pl.when(k == 2)
        def _():
            load_gu.wait()
            gate_own(0)

        @pl.when(k >= 3)
        def _():
            gate_rest(k - 2, False)

        arrive(0, k, 1, k < far - 1)
        arrive(1, k, 1, k < far)
        select(k, 1, False)

        @pl.when(k >= 2)
        def _():
            gate_own(k - 1)

        @pl.when(k == 2)
        def _():
            gate_rest(0, True)

        return carry

    lax.fori_loop(1, far, gather_step, 0)
    gate_own(far - 1)
    arrive(0, far, 0, None)
    arrive(1, far, 1, None)
    take_info(far, True)
    for h in range(2):
        select(far, h, True)
    gate_own(far)
    load_dn.wait()

    def rest_step(k, carry):
        gate_rest(k, False)
        return carry

    lax.fori_loop(far - 2, far, rest_step, 0)
    gate_rest(far, True)
    down(far - 1, False)
    down(far, True)

    def reduce_step(k, first, second):
        for way, h in ((0, 1), (1, 0), (0, 0), (1, 1)):
            if first and h != way:
                continue
            d = k if way == 0 else chips - k
            partial_copy(d, h).wait_recv()
            value = mine[d, h].astype(F32) + dd[d, h].astype(F32)
            if not first and not (second and h != way):
                sum_copy(way, k + 1, h).wait_recv()
                value = value + (rr if way == 0 else ll)[k, h].astype(F32)
            (sr if way == 0 else sl)[k - 1, h] = value.astype(BF16)
            sum_copy(way, k, h).start()

    reduce_step(far, True, False)
    reduce_step(far - 1, False, True)

    def tail_step(i, carry):
        k = far - 2 - i
        down(k, False)
        reduce_step(k, False, False)
        return carry

    lax.fori_loop(0, far - 2, tail_step, 0)
    down(0, True)
    for h in range(2):
        partial_copy(0, h).wait_recv()
        value = mine[0, h].astype(F32) + dd[0, h].astype(F32)
        sum_copy(0, 1, h).wait_recv()
        sum_copy(1, 1, h).wait_recv()
        value = value + rr[0, h].astype(F32) + ll[0, h].astype(F32)
        out_ref[:, h * half:(h + 1) * half] = value.astype(BF16)

    for d, cr in others:
        info_copy(d, cr).wait_send()
    for k in range(1, far + 1):
        for way in range(2):
            for h in range(2):
                if k < far or h == way:
                    gather_copy(way, k, h).wait_send()
                    sum_copy(way, k, h).wait_send()
    for k in range(far + 1):
        for o in range(1, n_seq):
            hidden_copy(k, o).wait_send()
            for h in range(2):
                rows_copy(k, h, o, k in (0, far)).wait_send()
    for d in range(chips):
        for h in range(2):
            twin_copy(d, h).wait_send()
            partial_copy(d, h).wait_send()


def body(n_seq, n_expert, tokens, expert_ids, route_weights, capacity, expert_gate_up, expert_down):
    group, share = tokens.shape
    half = share // 2
    hid, width = expert_gate_up.shape[2:]
    units = expert_down.shape[1]
    chips = n_expert // 2
    far = chips // 2
    lanes = -(-group // 128) * 128
    aligned = half % 128 == 0
    blocks = tokens if aligned else tokens.reshape(group, 2, half).transpose(1, 0, 2)
    sem = pltpu.SemaphoreType.DMA
    rows = 4 * CAP
    block = (group, half)
    return pl.pallas_call(
        functools.partial(kernel, n_seq, n_expert),
        out_shape=jax.ShapeDtypeStruct((group, share), BF16),
        in_specs=[
            pl.BlockSpec(memory_space=pltpu.VMEM),
            pl.BlockSpec(memory_space=pltpu.VMEM),
            pl.BlockSpec(memory_space=pltpu.SMEM),
            pl.BlockSpec(memory_space=pl.ANY),
            pl.BlockSpec(memory_space=pl.ANY),
            pl.BlockSpec(memory_space=pl.ANY),
        ],
        out_specs=pl.BlockSpec(memory_space=pltpu.VMEM),
        scratch_shapes=[
            pltpu.VMEM((2, hid, width), BF16),
            pltpu.VMEM((units, share), BF16),
            pltpu.VMEM((chips, 2, 2) + block, BF16),
            pltpu.VMEM((n_expert, 8, lanes), F32),
            pltpu.VMEM((chips, 2, 8, lanes), F32),
            pltpu.VMEM((far + 1, n_seq, 2, rows, half), BF16),
            pltpu.VMEM((far + 1, 2, rows, hid), F32),
            pltpu.VMEM((far + 1, n_seq, rows, hid), BF16),
            pltpu.VMEM((chips, 2) + block, BF16),
            pltpu.VMEM((chips, 2) + block, BF16),
            pltpu.VMEM((chips, 2) + block, BF16),
            pltpu.VMEM((far, 2) + block, BF16),
            pltpu.VMEM((far, 2) + block, BF16),
            pltpu.VMEM((far, 2) + block, BF16),
            pltpu.VMEM((far, 2) + block, BF16),
            sem((4,)),
            sem((chips, 2)), sem((chips, 2)),
            sem((2, far, 2)), sem((2, far, 2)),
            sem((chips, 2)), sem((chips, 2)),
            sem((far + 1, 2, max(1, n_seq - 1))), sem((far + 1, 2, max(1, n_seq - 1))),
            sem((far + 1, max(1, n_seq - 1))), sem((far + 1, max(1, n_seq - 1))),
            sem((chips, 2)), sem((chips, 2)),
            sem((2, far, 2)), sem((2, far, 2)),
        ],
        compiler_params=pltpu.CompilerParams(
            collective_id=0, has_side_effects=True, vmem_limit_bytes=60 * 1024 * 1024
        ),
    )(expert_ids.T, route_weights.T, capacity, blocks, expert_gate_up[0], expert_down[0])


def solution(mesh):
    in_specs = (
        P("expert", "seq"),
        P("expert", None),
        P("expert", None),
        P(),
        P("expert", None, "seq", None),
        P("expert", None, "seq"),
    )
    return jax.shard_map(
        functools.partial(body, mesh.shape["seq"], mesh.shape["expert"]),
        mesh=mesh, in_specs=in_specs, out_specs=P("expert", "seq"), check_vma=False,
    )
```

```python
import functools

import jax
import jax.numpy as jnp
from jax import lax
from jax.experimental import pallas as pl
from jax.experimental.pallas import tpu as pltpu
from jax.sharding import PartitionSpec as P

CAP = 12
MESH = pl.DeviceIdType.MESH
F32 = jnp.float32
BF16 = jnp.bfloat16


def kernel(
    n_seq, n_expert, ids_ref, weight_ref, cap_ref, tokens_ref, gate_up_ref, down_ref, out_ref,
    wgu, wdn, tok, table, info, xr, acc, hb, mine, pout, dd, sr, sl, rr, ll,
    local_sem, info_s, info_r, ag_s, ag_r, tw_s, tw_r, x_s, x_r, h_s, h_r, p_s, p_r, rs_s, rs_r,
):
    chips = n_expert // 2
    far = chips // 2
    group, half = tok.shape[3], tok.shape[4]
    share = 2 * half
    hid = wgu.shape[1]
    rows = xr.shape[3]
    small = -(-2 * CAP // 16) * 16
    aligned = half % 128 == 0
    me_e = lax.axis_index("expert")
    me_s = lax.axis_index("seq")
    core = lax.rem(me_e, 2)
    chip = lax.div(me_e, 2)
    odd = lax.rem(chip, 2)
    pos = (1 - odd) * lax.div(chip, 2) + odd * (chips - 1 - lax.div(chip, 2))

    def device_at(offset, same_core):
        at = lax.rem(pos + offset + 2 * chips, chips)
        back = lax.div(at, far)
        there = (1 - back) * 2 * at + back * (2 * (chips - 1 - at) + 1)
        return there * 2 + (core if same_core else 1 - core)

    right, left, twin = device_at(1, True), device_at(-1, True), device_at(0, False)

    def remote(src, dst, send, recv, device):
        return pltpu.make_async_remote_copy(
            src_ref=src, dst_ref=dst, send_sem=send, recv_sem=recv,
            device_id=device, device_id_type=MESH,
        )

    def info_copy(d, cr):
        to = device_at(-d, cr == 0)
        return remote(table.at[to], info.at[d, cr], info_s.at[d, cr], info_r.at[d, cr], {"expert": to})

    def gather_copy(way, k, h):
        src = lax.rem(chips - k + 1, chips) if way == 0 else k - 1
        dst = chips - k if way == 0 else k
        return remote(
            tok.at[src, 0, h], tok.at[dst, 0, h], ag_s.at[way, k - 1, h], ag_r.at[way, k - 1, h],
            {"expert": right if way == 0 else left},
        )

    def twin_copy(d, h):
        return remote(tok.at[d, 0, h], tok.at[d, 1, h], tw_s.at[d, h], tw_r.at[d, h], {"expert": twin})

    def rows_copy(k, h, o, single, receive=False):
        slot = lax.rem(me_s - o + n_seq, n_seq) if receive else me_s
        span = xr.at[k, slot, h, pl.ds(0, small)] if single else xr.at[k, slot, h]
        return remote(
            span, span, x_s.at[k, h, o - 1], x_r.at[k, h, o - 1], {"seq": lax.rem(me_s + o, n_seq)}
        )

    def hidden_copy(k, o, receive=False):
        slot = lax.rem(me_s - o + n_seq, n_seq) if receive else me_s
        return remote(
            hb.at[k, slot], hb.at[k, slot], h_s.at[k, o - 1], h_r.at[k, o - 1],
            {"seq": lax.rem(me_s + o, n_seq)},
        )

    def partial_copy(d, h):
        return remote(pout.at[d, h], dd.at[d, h], p_s.at[d, h], p_r.at[d, h], {"expert": twin})

    def sum_copy(way, k, h):
        src, dst = (sr, rr) if way == 0 else (sl, ll)
        return remote(
            src.at[k - 1, h], dst.at[k - 1, h], rs_s.at[way, k - 1, h], rs_r.at[way, k - 1, h],
            {"expert": right if way == 0 else left},
        )

    if aligned:
        load_tokens = [
            pltpu.make_async_copy(
                tokens_ref.at[:, pl.ds(h * half, half)], tok.at[0, 0, h], local_sem.at[h]
            )
            for h in range(2)
        ]
    else:
        load_tokens = [pltpu.make_async_copy(tokens_ref, tok.at[0, 0], local_sem.at[0])]
    load_gu = pltpu.make_async_copy(gate_up_ref, wgu, local_sem.at[2])
    load_dn = pltpu.make_async_copy(down_ref, wdn, local_sem.at[3])
    for load in load_tokens:
        load.start()
    load_gu.start()
    load_dn.start()

    barrier = pltpu.get_barrier_semaphore()
    for o in range(1, n_expert):
        pl.semaphore_signal(
            barrier, inc=1, device_id={"expert": lax.rem(me_e + o, n_expert)}, device_id_type=MESH
        )
    for o in range(1, n_seq):
        pl.semaphore_signal(
            barrier, inc=1, device_id={"seq": lax.rem(me_s + o, n_seq)}, device_id_type=MESH
        )
    expert_at = lax.broadcasted_iota(jnp.int32, (n_expert, group), 0)
    weight = jnp.zeros((n_expert, group), F32)
    chosen = jnp.zeros((n_expert, group), F32)
    for c in range(ids_ref.shape[0]):
        hit = expert_at == ids_ref[c:c + 1, :]
        weight = weight + jnp.where(hit, weight_ref[c:c + 1, :], 0.0)
        chosen = chosen + jnp.where(hit, 1.0, 0.0)
    before = lax.broadcasted_iota(jnp.int32, (group, group), 0)
    after = lax.broadcasted_iota(jnp.int32, (group, group), 1)
    earlier = jnp.where(before < after, 1.0, 0.0).astype(BF16)
    rank = jnp.dot(chosen.astype(BF16), earlier, preferred_element_type=F32)
    limit = jnp.zeros((n_expert, group), jnp.int32)
    for e in range(n_expert):
        limit = jnp.where(expert_at == e, cap_ref[e], limit)
    keep = jnp.logical_and(chosen > 0.5, rank < limit.astype(F32))
    weight = jnp.where(keep, weight, 0.0)
    rank = jnp.where(keep, rank, -10000.0)
    for e in range(n_expert):
        table[e, 0:1, :group] = weight[e:e + 1]
        table[e, 1:2, :group] = rank[e:e + 1]
    info[0, 0] = table[me_e]
    for k in (0, far):
        for s in range(n_seq):
            for h in range(2):
                xr[k, s, h, small:] = jnp.zeros((rows - small, half), BF16)
    for load in load_tokens:
        load.wait()
    pl.semaphore_wait(barrier, n_expert - 1 + n_seq - 1)

    others = [(d, cr) for d in range(chips) for cr in range(2) if d or cr]
    others.sort(key=lambda at: min(at[0], chips - at[0]))
    near = [at for at in others if min(at[0], chips - at[0]) <= 1]
    for d, cr in near:
        info_copy(d, cr).start()
    for way, h in ((0, 0), (1, 0), (0, 1), (1, 1)):
        gather_copy(way, 1, h).start()
    for h in range(2):
        twin_copy(0, h).start()
    for d, cr in others[len(near):]:
        info_copy(d, cr).start()

    def distances(k, single):
        return (k,) if single else (k, chips - k)

    def slots_of(k, single, weighted, height):
        parts = []
        for d in distances(k, single):
            for cr in range(2):
                block = info[d, cr]
                row = lax.broadcasted_iota(jnp.int32, (height, group), 0).astype(F32)
                hit = row == block[1:2, :group] + float(CAP * len(parts))
                parts.append(jnp.where(hit, block[0:1, :group] if weighted else 1.0, 0.0))
        return jnp.concatenate(parts, axis=1)

    def select(k, h, single):
        height = small if single else rows
        placing = slots_of(k, single, False, height).astype(BF16)
        for d in distances(k, single):
            twin_copy(d, h).wait_recv()
        block = jnp.concatenate([tok[d, cr, h] for d in distances(k, single) for cr in range(2)], axis=0)
        xr[k, me_s, h, :height] = jnp.dot(placing, block, preferred_element_type=F32).astype(BF16)
        for o in range(1, n_seq):
            rows_copy(k, h, o, single).start()

    def take_info(k, single):
        for d in distances(k, single):
            info_copy(d, 1).wait_recv()
            if not (single and isinstance(d, int) and d == 0):
                info_copy(d, 0).wait_recv()

    def block_sum(k, s, dynamic):
        total = None
        for h in range(2):
            at = s * share + h * half
            columns = pl.ds(pl.multiple_of(at, 128), half) if dynamic else slice(at, at + half)
            term = [
                lax.dot_general(
                    xr[k, s, h], wgu[g, :, columns], (((1,), (1,)), ((), ())),
                    preferred_element_type=F32,
                )
                for g in range(2)
            ]
            total = term if total is None else [a + b for a, b in zip(total, term)]
        return [a.astype(BF16).astype(F32) for a in total]

    def gate_own(k):
        if aligned:
            own = block_sum(k, me_s, True)
            for g in range(2):
                acc[k, g] = own[g]

    def gate_rest(k, single):
        for o in range(1, n_seq):
            for h in range(2):
                rows_copy(k, h, o, single, True).wait_recv()
        if aligned:
            total = [acc[k, g] for g in range(2)]
            for o in range(1, n_seq):
                more = block_sum(k, lax.rem(me_s - o + n_seq, n_seq), True)
                total = [a + b for a, b in zip(total, more)]
        else:
            total = block_sum(k, 0, False)
            for s in range(1, n_seq):
                total = [a + b for a, b in zip(total, block_sum(k, s, False))]
        value = total[0] / (1.0 + jnp.exp(-total[0])) * total[1]
        hb[k, me_s] = value.astype(BF16)
        for o in range(1, n_seq):
            hidden_copy(k, o).start()

    def down(k, single):
        for o in range(1, n_seq):
            hidden_copy(k, o, True).wait_recv()
        mixing = slots_of(k, single, True, rows).T.astype(BF16)
        for h in range(2):
            value = None
            for s in range(n_seq):
                term = jnp.dot(
                    hb[k, s], wdn[s * hid:(s + 1) * hid, h * half:(h + 1) * half],
                    preferred_element_type=F32,
                )
                value = term if value is None else value + term
            mixed = jnp.dot(mixing, value.astype(BF16), preferred_element_type=F32).astype(BF16)
            for j, d in enumerate(distances(k, single)):
                mine[d, h] = mixed[2 * j * group:(2 * j + 1) * group]
                pout[d, h] = mixed[(2 * j + 1) * group:(2 * j + 2) * group]
                partial_copy(d, h).start()

    def arrive(way, k, h, forward):
        gather_copy(way, k, h).wait_recv()
        if forward is not None:
            @pl.when(forward)
            def _():
                gather_copy(way, k + 1, h).start()
        twin_copy(chips - k if way == 0 else k, h).start()

    take_info(0, True)
    for h in range(2):
        select(0, h, True)

    def gather_step(k, carry):
        arrive(0, k, 0, k < far)
        arrive(1, k, 0, k < far - 1)
        take_info(k, False)
        select(k, 0, False)

        @pl.when(k == 2)
        def _():
            load_gu.wait()
            gate_own(0)

        @pl.when(k >= 3)
        def _():
            gate_rest(k - 2, False)

        arrive(0, k, 1, k < far - 1)
        arrive(1, k, 1, k < far)
        select(k, 1, False)

        @pl.when(k >= 2)
        def _():
            gate_own(k - 1)

        return carry

    lax.fori_loop(1, far, gather_step, 0)
    gate_own(far - 1)
    arrive(0, far, 0, None)
    arrive(1, far, 1, None)
    take_info(far, True)
    for h in range(2):
        select(far, h, True)
    gate_own(far)
    load_dn.wait()

    def rest_step(k, carry):
        gate_rest(k, False)
        return carry

    lax.fori_loop(far - 2, far, rest_step, 0)
    gate_rest(far, True)
    down(far - 1, False)
    down(far, True)

    def reduce_step(k, fresh, held):
        for way, h in [(0, 1), (1, 0)] * fresh + [(0, 0), (1, 1)] * held:
            d = k if way == 0 else chips - k
            partial_copy(d, h).wait_recv()
            value = mine[d, h].astype(F32) + dd[d, h].astype(F32)
            starts = isinstance(k, int) and (k == far or (k == far - 1 and h != way))
            if not starts:
                sum_copy(way, k + 1, h).wait_recv()
                value = value + (rr if way == 0 else ll)[k, h].astype(F32)
            (sr if way == 0 else sl)[k - 1, h] = value.astype(BF16)
            sum_copy(way, k, h).start()

    reduce_step(far, False, True)
    reduce_step(far - 1, True, False)
    down(far - 2, False)
    reduce_step(far - 1, False, True)

    def tail_step(i, carry):
        k = far - 2 - i
        down(k - 1, False)
        reduce_step(k, True, True)
        return carry

    lax.fori_loop(0, far - 3, tail_step, 0)
    gate_rest(0, True)
    reduce_step(1, True, True)
    down(0, True)
    for h in range(2):
        partial_copy(0, h).wait_recv()
        value = mine[0, h].astype(F32) + dd[0, h].astype(F32)
        sum_copy(0, 1, h).wait_recv()
        sum_copy(1, 1, h).wait_recv()
        value = value + rr[0, h].astype(F32) + ll[0, h].astype(F32)
        out_ref[:, h * half:(h + 1) * half] = value.astype(BF16)

    for d, cr in others:
        info_copy(d, cr).wait_send()
    for k in range(1, far + 1):
        for way in range(2):
            for h in range(2):
                if k < far or h == way:
                    gather_copy(way, k, h).wait_send()
                    sum_copy(way, k, h).wait_send()
    for k in range(far + 1):
        for o in range(1, n_seq):
            hidden_copy(k, o).wait_send()
            for h in range(2):
                rows_copy(k, h, o, k in (0, far)).wait_send()
    for d in range(chips):
        for h in range(2):
            twin_copy(d, h).wait_send()
            partial_copy(d, h).wait_send()


def body(n_seq, n_expert, tokens, expert_ids, route_weights, capacity, expert_gate_up, expert_down):
    group, share = tokens.shape
    half = share // 2
    hid, width = expert_gate_up.shape[2:]
    units = expert_down.shape[1]
    chips = n_expert // 2
    far = chips // 2
    lanes = -(-group // 128) * 128
    aligned = half % 128 == 0
    blocks = tokens if aligned else tokens.reshape(group, 2, half).transpose(1, 0, 2)
    sem = pltpu.SemaphoreType.DMA
    rows = 4 * CAP
    block = (group, half)
    return pl.pallas_call(
        functools.partial(kernel, n_seq, n_expert),
        out_shape=jax.ShapeDtypeStruct((group, share), BF16),
        in_specs=[
            pl.BlockSpec(memory_space=pltpu.VMEM),
            pl.BlockSpec(memory_space=pltpu.VMEM),
            pl.BlockSpec(memory_space=pltpu.SMEM),
            pl.BlockSpec(memory_space=pl.ANY),
            pl.BlockSpec(memory_space=pl.ANY),
            pl.BlockSpec(memory_space=pl.ANY),
        ],
        out_specs=pl.BlockSpec(memory_space=pltpu.VMEM),
        scratch_shapes=[
            pltpu.VMEM((2, hid, width), BF16),
            pltpu.VMEM((units, share), BF16),
            pltpu.VMEM((chips, 2, 2) + block, BF16),
            pltpu.VMEM((n_expert, 8, lanes), F32),
            pltpu.VMEM((chips, 2, 8, lanes), F32),
            pltpu.VMEM((far + 1, n_seq, 2, rows, half), BF16),
            pltpu.VMEM((far + 1, 2, rows, hid), F32),
            pltpu.VMEM((far + 1, n_seq, rows, hid), BF16),
            pltpu.VMEM((chips, 2) + block, BF16),
            pltpu.VMEM((chips, 2) + block, BF16),
            pltpu.VMEM((chips, 2) + block, BF16),
            pltpu.VMEM((far, 2) + block, BF16),
            pltpu.VMEM((far, 2) + block, BF16),
            pltpu.VMEM((far, 2) + block, BF16),
            pltpu.VMEM((far, 2) + block, BF16),
            sem((4,)),
            sem((chips, 2)), sem((chips, 2)),
            sem((2, far, 2)), sem((2, far, 2)),
            sem((chips, 2)), sem((chips, 2)),
            sem((far + 1, 2, max(1, n_seq - 1))), sem((far + 1, 2, max(1, n_seq - 1))),
            sem((far + 1, max(1, n_seq - 1))), sem((far + 1, max(1, n_seq - 1))),
            sem((chips, 2)), sem((chips, 2)),
            sem((2, far, 2)), sem((2, far, 2)),
        ],
        compiler_params=pltpu.CompilerParams(
            collective_id=0, has_side_effects=True, vmem_limit_bytes=60 * 1024 * 1024
        ),
    )(expert_ids.T, route_weights.T, capacity, blocks, expert_gate_up[0], expert_down[0])


def solution(mesh):
    in_specs = (
        P("expert", "seq"),
        P("expert", None),
        P("expert", None),
        P(),
        P("expert", None, "seq", None),
        P("expert", None, "seq"),
    )
    return jax.shard_map(
        functools.partial(body, mesh.shape["seq"], mesh.shape["expert"]),
        mesh=mesh, in_specs=in_specs, out_specs=P("expert", "seq"), check_vma=False,
    )
```
